32 devices in a mesh: north: 4 (over y, x), east: 8 (over z, core).
Axes of the slice: x: 2, y: 2, z: 4, core: 2. Of those that a mesh axis runs over, the one named last changes fastest.
Arguments:
- pair_rows: bfloat16 [96, 96, 128], P('north', 'east'), may hold values from -6 to 6
- in_gain: float32 [128], replicated, may hold values from 0.25 to 1.75
- left_weight: bfloat16 [128, 128], replicated, may hold values from -0.5 to 0.5
- right_weight: bfloat16 [128, 128], replicated, may hold values from -0.5 to 0.5
- left_gate: bfloat16 [128, 128], replicated, may hold values from -0.5 to 0.5
- right_gate: bfloat16 [128, 128], replicated, may hold values from -0.5 to 0.5
- mid_gain: float32 [128], replicated, may hold values from 0.25 to 1.75
- out_weight: bfloat16 [128, 128], replicated, may hold values from -0.5 to 0.5
- out_gate: bfloat16 [128, 128], replicated, may hold values from -0.5 to 0.5
Outputs:
- pair_change: bfloat16 [96, 96, 128], P('north', 'east')
The draws below stay inside these ranges and needn't reach their ends.
All inputs are finite; a program needn't handle non-finite values.
Results may differ from the reference program's by a relative error of at most 0.012.
Values may be sent and summed in bfloat16 or wider, within the bound.
A program may use at most 128 MiB of HBM per device.

```python
import jax
import jax.numpy as jnp
from jax import lax

RESIDUES = 96
PAIR_WIDTH = 128
MIX_WIDTH = 128


def levels(stream_key, shape, split, smallest, top_value):
    level = 1.0
    for dim, shards_of in split:
        draws = jax.random.uniform(jax.random.fold_in(jax.random.fold_in(stream_key, 6), dim), (shards_of,), jnp.float32, smallest / len(split), top_value / len(split))
        level = level * jnp.repeat(jnp.exp(draws), shape[dim] // shards_of).reshape((-1,) + (1,) * (len(shape) - 1 - dim))
    return level


def scatter_about(own_key, dims, width, most, split=(), dtype=jnp.bfloat16):
    entries = jax.random.normal(own_key, dims, jnp.float32) * width
    if len(split) > 0:
        entries = levels(own_key, dims, split, -0.22, 0.18) * entries
    return jnp.clip(entries, min=-most, max=most).astype(dtype)


def setup_inputs(seed: int = 0) -> dict:
    key_list = jax.random.split(jax.random.key(seed), 10)
    return {
        "pair_rows": scatter_about(key_list[0], (RESIDUES, RESIDUES, PAIR_WIDTH), 1.0, 6.0, ((0, 4), (1, 8))),
        "in_gain": jnp.clip(1.0 + 0.15 * jax.random.normal(key_list[1], (PAIR_WIDTH,), jnp.float32), 0.25, 1.75),
        "left_weight": scatter_about(key_list[2], (PAIR_WIDTH, MIX_WIDTH), PAIR_WIDTH ** -0.5, 0.5),
        "right_weight": scatter_about(key_list[3], (PAIR_WIDTH, MIX_WIDTH), PAIR_WIDTH ** -0.5, 0.5),
        "left_gate": scatter_about(key_list[4], (PAIR_WIDTH, MIX_WIDTH), PAIR_WIDTH ** -0.5, 0.5),
        "right_gate": scatter_about(key_list[5], (PAIR_WIDTH, MIX_WIDTH), PAIR_WIDTH ** -0.5, 0.5),
        "mid_gain": jnp.clip(1.0 + 0.15 * jax.random.normal(key_list[6], (MIX_WIDTH,), jnp.float32), 0.25, 1.75),
        "out_weight": scatter_about(key_list[7], (MIX_WIDTH, PAIR_WIDTH), MIX_WIDTH ** -0.5, 0.5),
        "out_gate": scatter_about(key_list[8], (PAIR_WIDTH, PAIR_WIDTH), PAIR_WIDTH ** -0.5, 0.5),
    }


def scale_channels(values, channel_gain):
    centred = values - lax.optimization_barrier(jnp.mean(values, axis=-1, keepdims=True))
    return centred * lax.rsqrt(lax.optimization_barrier(jnp.mean(centred * centred, axis=-1, keepdims=True)) + 1e-05) * channel_gain

def both_factors(pair_in, in_gain, left_weight, right_weight, left_gate, right_gate):
    ready = scale_channels(pair_in.astype(jnp.float32), in_gain).astype(jnp.bfloat16)
    ready = lax.optimization_barrier(ready)
    left = jnp.einsum('ijc,cd->ijd', ready.astype(jnp.float32), left_weight.astype(jnp.float32))
    left = left * jax.nn.sigmoid(jnp.einsum('ijc,cd->ijd', ready.astype(jnp.float32), left_gate.astype(jnp.float32)))
    right = jnp.einsum('ijc,cd->ijd', ready.astype(jnp.float32), right_weight.astype(jnp.float32))
    right = right * jax.nn.sigmoid(jnp.einsum('ijc,cd->ijd', ready.astype(jnp.float32), right_gate.astype(jnp.float32)))
    return (ready, left.astype(jnp.bfloat16), right.astype(jnp.bfloat16))

def to_pair(mixed, ready, mid_gain, out_weight, out_gate):
    scaled = scale_channels(mixed.astype(jnp.float32), mid_gain).astype(jnp.bfloat16)
    scaled = lax.optimization_barrier(scaled)
    gate = jax.nn.sigmoid(jnp.einsum('ijc,cd->ijd', ready.astype(jnp.float32), out_gate.astype(jnp.float32)))
    return (jnp.einsum('ijd,dc->ijc', scaled.astype(jnp.float32), out_weight.astype(jnp.float32)) * gate).astype(jnp.bfloat16)

def reference(pair_rows, in_gain, left_weight, right_weight, left_gate, right_gate, mid_gain, out_weight, out_gate):
    ready, left, right = both_factors(pair_rows, in_gain, left_weight, right_weight, left_gate, right_gate)
    left, right = lax.optimization_barrier((left, right))

    def one_channel(pair_of):
        return (jnp.dot(pair_of[0].T, pair_of[1], preferred_element_type=jnp.float32) * RESIDUES ** (-0.5)).astype(jnp.bfloat16)
    mixed = jnp.moveaxis(lax.map(one_channel, (jnp.moveaxis(left, -1, 0), jnp.moveaxis(right, -1, 0))), 0, -1)
    mixed = lax.optimization_barrier(mixed)
    return to_pair(mixed, ready, mid_gain, out_weight, out_gate)
```

```python
import functools

import jax
import jax.numpy as jnp
from jax import lax
from jax.experimental import pallas as pl
from jax.experimental.pallas import tpu as pltpu
from jax.sharding import PartitionSpec as P

MESH = pl.DeviceIdType.MESH
F32 = jnp.float32
BF16 = jnp.bfloat16
LANES = 8


def scale_channels(values, channel_gain):
    centred = values - jnp.mean(values, axis=-1, keepdims=True)
    return (
        centred
        * lax.rsqrt(jnp.mean(centred * centred, axis=-1, keepdims=True) + 1e-05)
        * channel_gain
    )


def nearest_first(chips):
    return [sorted(range(chips), key=lambda other: (abs(other - z), other)) for z in range(chips)]


def kernel(
    norths,
    easts,
    lines,
    columns,
    pair_hbm,
    in_gain_hbm,
    left_weight_hbm,
    right_weight_hbm,
    left_gate_hbm,
    right_gate_hbm,
    mid_gain_hbm,
    out_weight_hbm,
    out_gate_hbm,
    out_ref,
    pair_in,
    gains,
    weights,
    rows32,
    ready_ref,
    gate_ref,
    left_all,
    left32,
    right_own,
    right_partner,
    right32,
    sums32,
    sums_dense,
    sums_send,
    sums_all,
    load_sem,
    left_send_sem,
    left_recv_sem,
    right_sem,
    sums_send_sem,
    sums_recv_sem,
):
    rows, width = pair_in.shape
    chips = easts // 2
    ratio = lines // columns
    piece = columns * columns

    north = lax.axis_index("north")
    east = lax.axis_index("east")
    chip = east // 2
    core = east % 2
    partner = chip * 2 + 1 - core

    loads = [
        (pair_hbm, pair_in),
        (in_gain_hbm, gains.at[pl.ds(0, 1)]),
        (left_weight_hbm, weights.at[0]),
        (left_gate_hbm, weights.at[1]),
        (right_weight_hbm, weights.at[2]),
        (right_gate_hbm, weights.at[3]),
        (out_gate_hbm, weights.at[4]),
        (out_weight_hbm, weights.at[5]),
        (mid_gain_hbm, gains.at[pl.ds(8, 1)]),
    ]
    loads = [
        pltpu.make_async_copy(source, target, load_sem.at[at])
        for at, (source, target) in enumerate(loads)
    ]
    for load in loads:
        load.start()

    barrier = pltpu.get_barrier_semaphore()
    for step in range(1, chips):
        there = lax.rem(chip + step, chips)
        pl.semaphore_signal(
            barrier, inc=1, device_id=(north, there * 2 + core), device_id_type=MESH
        )
    for step in range(norths):
        there = lax.rem(north + step, norths)
        if step:
            pl.semaphore_signal(barrier, inc=1, device_id=(there, east), device_id_type=MESH)
        pl.semaphore_signal(barrier, inc=1, device_id=(there, partner), device_id_type=MESH)

    table = nearest_first(chips)
    order = []
    for step in range(1, chips):
        other = jnp.int32(0)
        for z in range(chips):
            other = other + (chip == z).astype(jnp.int32) * table[z][step]
        order.append(other)

    loads[0].wait()
    loads[1].wait()

    chunk = rows // max(1, rows // 288)
    if rows % chunk or chunk % 16:
        chunk = rows

    def in_chunks(step):
        if chunk == rows:
            step(pl.ds(0, rows))
        else:

            @pl.loop(0, rows // chunk)
            def _(at):
                step(pl.ds(pl.multiple_of(at * chunk, chunk), chunk))

    def project(ready, which):
        return jnp.dot(ready, weights[which], preferred_element_type=F32)

    loads[2].wait()
    loads[3].wait()

    def left_chunk(part):
        ready = scale_channels(pair_in[part, :].astype(F32), gains[pl.ds(0, 1), :]).astype(BF16)
        ready_ref[part, :] = ready
        left = project(ready, 0) * jax.nn.sigmoid(project(ready, 1))
        left_all[chip, part, :] = left.astype(BF16)

    in_chunks(left_chunk)
    pl.semaphore_wait(barrier, chips - 1 + 2 * norths - 1)

    left_copies = []
    for step in reversed(range(chips - 1)):
        copy = pltpu.make_async_remote_copy(
            src_ref=left_all.at[chip],
            dst_ref=left_all.at[chip],
            send_sem=left_send_sem.at[step],
            recv_sem=left_recv_sem.at[chip],
            device_id=(north, order[step] * 2 + core),
            device_id_type=MESH,
        )
        copy.start()
        left_copies.append(copy)

    loads[4].wait()
    loads[5].wait()

    def right_chunk(part):
        ready = ready_ref[part, :]
        right = project(ready, 2) * jax.nn.sigmoid(project(ready, 3))
        right = right.astype(BF16)
        right_own[part, :] = right
        rows32[part, :] = right.astype(F32)

    in_chunks(right_chunk)
    right_copy = pltpu.make_async_remote_copy(
        src_ref=right_own,
        dst_ref=right_partner,
        send_sem=right_sem.at[0],
        recv_sem=right_sem.at[1],
        device_id=(north, partner),
        device_id_type=MESH,
    )
    right_copy.start()
    for line in range(lines):
        right32[line, pl.ds(0, columns), :] = rows32[pl.ds(line, columns, stride=lines), :]

    loads[6].wait()

    def gate_chunk(part):
        gate_ref[part, :] = jax.nn.sigmoid(project(ready_ref[part, :], 4))

    in_chunks(gate_chunk)

    right_copy.wait()
    rows32[...] = right_partner[...].astype(F32)
    for line in range(lines):
        right32[line, pl.ds(columns, columns), :] = rows32[pl.ds(line, columns, stride=lines), :]

    tiles = 2 * columns // LANES
    group = max(g for g in range(1, columns + 1) if columns % g == 0 and (g * tiles <= 36 or g == 1))

    def partial_sums(which):
        left32[...] = left_all[which].astype(F32)
        for first in range(0, columns, group):

            def term(line, totals):
                rights = [right32[line, pl.ds(LANES * t, LANES), :] for t in range(tiles)]
                new = []
                for i in range(group):
                    row = left32[pl.ds((first + i) * lines + line, LANES, stride=0), :]
                    for t in range(tiles):
                        new.append(totals[i * tiles + t] + row * rights[t])
                return tuple(new)

            zero = jnp.zeros((LANES, width), F32)
            totals = lax.fori_loop(0, lines, term, (zero,) * (group * tiles))
            for i in range(group):
                for t in range(tiles):
                    at = (first + i) * 2 * columns + LANES * t
                    sums32[pl.ds(at, LANES), :] = totals[i * tiles + t]
        for half in range(2):
            for j in range(columns):
                sums_dense[half, pl.ds(j * columns, columns), :] = sums32[
                    pl.ds(half * columns + j, columns, stride=2 * columns), :
                ]

    def sums_copy(step, half, owner, block):
        return pltpu.make_async_remote_copy(
            src_ref=sums_send.at[step, half],
            dst_ref=sums_all.at[north, block],
            send_sem=sums_send_sem.at[step, half],
            recv_sem=sums_recv_sem.at[north, block],
            device_id=(owner, partner if half else east),
            device_id_type=MESH,
        )

    sent = []
    for step in range(chips):
        source = chip if step == 0 else order[step - 1]
        if step:
            pltpu.make_async_remote_copy(
                src_ref=left_all.at[source],
                dst_ref=left_all.at[source],
                send_sem=left_send_sem.at[step - 1],
                recv_sem=left_recv_sem.at[source],
                device_id=(north, source * 2 + core),
                device_id_type=MESH,
            ).wait_recv()
        partial_sums(source)
        owner = (source * 2 + core) // ratio
        block = (source * 2 + core) % ratio
        sums_send[step, 1] = sums_dense[1].astype(BF16)
        sums_copy(step, 1, owner, block).start()
        here = owner == north

        @pl.when(here)
        def _():
            sums_all[north, block] = sums_dense[0].astype(BF16)

        @pl.when(jnp.logical_not(here))
        def _():
            sums_send[step, 0] = sums_dense[0].astype(BF16)
            sums_copy(step, 0, owner, block).start()

        sent.append((owner, block, here))

    for copy in left_copies:
        copy.wait_send()
    for step, (owner, block, here) in enumerate(sent):
        sums_copy(step, 1, owner, block).wait_send()

        @pl.when(jnp.logical_not(here))
        def _():
            sums_copy(step, 0, owner, block).wait_send()

    loads[7].wait()
    loads[8].wait()
    for block in range(ratio):
        for ahead in range(norths):
            origin = lax.rem(north + ahead, norths)
            arrival = pltpu.make_async_remote_copy(
                src_ref=sums_send.at[0, 0],
                dst_ref=sums_all.at[origin, block],
                send_sem=sums_send_sem.at[0, 0],
                recv_sem=sums_recv_sem.at[origin, block],
                device_id=(origin, partner),
                device_id_type=MESH,
            )
            if ahead:
                arrival.wait_recv()
            else:

                @pl.when(core != block % 2)
                def _():
                    arrival.wait_recv()

        total = sums_all[0, block].astype(F32)
        for origin in range(1, norths):
            total = total + sums_all[origin, block].astype(F32)
        sums32[pl.ds(0, piece), :] = total
        for j in range(columns):
            rows32[pl.ds(j * lines + block * columns, columns), :] = sums32[
                pl.ds(j * columns, columns), :
            ]

    def out_chunk(part):
        mixed = (rows32[part, :] * (lines * norths) ** (-0.5)).astype(BF16).astype(F32)
        scaled = scale_channels(mixed, gains[pl.ds(8, 1), :]).astype(BF16)
        out_ref[part, :] = (project(scaled, 5) * gate_ref[part, :]).astype(BF16)

    in_chunks(out_chunk)


def body(pair_rows, in_gain, left_weight, right_weight, left_gate, right_gate, mid_gain, out_weight, out_gate):
    lines, columns, width = pair_rows.shape
    norths, easts = lax.axis_size("north"), lax.axis_size("east")
    rows = lines * columns
    chips, ratio, piece = easts // 2, lines // columns, columns * columns
    dma = pltpu.SemaphoreType.DMA
    out = pl.pallas_call(
        functools.partial(kernel, norths, easts, lines, columns),
        out_shape=jax.ShapeDtypeStruct((rows, width), BF16),
        in_specs=[pl.BlockSpec(memory_space=pl.ANY)] * 9,
        out_specs=pl.BlockSpec(memory_space=pltpu.VMEM),
        scratch_shapes=[
            pltpu.VMEM((rows, width), BF16),
            pltpu.VMEM((16, width), F32),
            pltpu.VMEM((6, width, width), BF16),
            pltpu.VMEM((rows, width), F32),
            pltpu.VMEM((rows, width), BF16),
            pltpu.VMEM((rows, width), F32),
            pltpu.VMEM((chips, rows, width), BF16),
            pltpu.VMEM((rows, width), F32),
            pltpu.VMEM((rows, width), BF16),
            pltpu.VMEM((rows, width), BF16),
            pltpu.VMEM((lines, 2 * columns, width), F32),
            pltpu.VMEM((columns * 2 * columns, width), F32),
            pltpu.VMEM((2, piece, width), F32),
            pltpu.VMEM((chips, 2, piece, width), BF16),
            pltpu.VMEM((norths, ratio, piece, width), BF16),
            dma((9,)),
            dma((chips - 1,)),
            dma((chips,)),
            dma((2,)),
            dma((chips, 2)),
            dma((norths, ratio)),
        ],
        compiler_params=pltpu.CompilerParams(collective_id=0, has_side_effects=True),
        name="triangle",
    )(
        pair_rows.transpose(1, 0, 2).reshape(rows, width),
        in_gain.reshape(1, -1),
        left_weight,
        right_weight,
        left_gate,
        right_gate,
        mid_gain.reshape(1, -1),
        out_weight,
        out_gate,
    )
    return out.reshape(columns, lines, width).transpose(1, 0, 2)


def solution(mesh):
    placed = (P("north", "east", None), P(), P(), P(), P(), P(), P(), P(), P())
    return jax.shard_map(
        body, mesh=mesh, in_specs=placed, out_specs=P("north", "east", None), check_vma=False
    )
```

```python
import functools

import jax
import jax.numpy as jnp
from jax import lax
from jax.experimental import pallas as pl
from jax.experimental.pallas import tpu as pltpu
from jax.sharding import PartitionSpec as P

MESH = pl.DeviceIdType.MESH
F32 = jnp.float32
BF16 = jnp.bfloat16
LANES = 8


def scale_channels(values, channel_gain):
    centred = values - jnp.mean(values, axis=-1, keepdims=True)
    return (
        centred
        * lax.rsqrt(jnp.mean(centred * centred, axis=-1, keepdims=True) + 1e-05)
        * channel_gain
    )


def pieces_of(lines, columns):
    for pieces in (1,):
        if columns % pieces == 0 and all(
            columns // pieces * side % 16 == 0 for side in (lines, columns)
        ):
            return pieces
    return 1


def kernel(
    norths,
    easts,
    lines,
    columns,
    pair_hbm,
    in_gain_hbm,
    left_weight_hbm,
    right_weight_hbm,
    left_gate_hbm,
    right_gate_hbm,
    mid_gain_hbm,
    out_weight_hbm,
    out_gate_hbm,
    out_ref,
    pair_in,
    gains,
    weights,
    rows32,
    ready_ref,
    gate_ref,
    left_all,
    left32,
    right_own,
    right_partner,
    right32,
    sums32,
    sums_dense,
    sums_send,
    sums_all,
    load_sem,
    left_send_sem,
    left_recv_sem,
    right_sem,
    sums_send_sem,
    sums_recv_sem,
):
    rows, width = pair_in.shape
    chips = easts // 2
    ratio = lines // columns
    pieces = pieces_of(lines, columns)
    deep = columns // pieces
    left_rows, sum_rows = deep * lines, deep * columns

    north = lax.axis_index("north")
    east = lax.axis_index("east")
    chip = east // 2
    core = east % 2
    partner = chip * 2 + 1 - core

    loads = [
        (pair_hbm, pair_in),
        (in_gain_hbm, gains.at[pl.ds(0, 1)]),
        (left_weight_hbm, weights.at[0]),
        (left_gate_hbm, weights.at[1]),
        (right_weight_hbm, weights.at[2]),
        (right_gate_hbm, weights.at[3]),
        (out_gate_hbm, weights.at[4]),
        (out_weight_hbm, weights.at[5]),
        (mid_gain_hbm, gains.at[pl.ds(8, 1)]),
    ]
    loads = [
        pltpu.make_async_copy(source, target, load_sem.at[at])
        for at, (source, target) in enumerate(loads)
    ]
    for load in loads:
        load.start()

    barrier = pltpu.get_barrier_semaphore()
    routes = [(up, far) for far in (2, 1) for up in range(2)]

    def reached(up, far):
        return chip + far if up else chip - far

    def exists(up, far):
        return reached(up, far) < chips if up else reached(up, far) >= 0

    for up, far in routes:

        @pl.when(exists(up, far))
        def _():
            pl.semaphore_signal(
                barrier,
                inc=1,
                device_id=(north, reached(up, far) * 2 + core),
                device_id_type=MESH,
            )

    for step in range(norths):
        there = lax.rem(north + step, norths)
        if step:
            pl.semaphore_signal(barrier, inc=1, device_id=(there, east), device_id_type=MESH)
        pl.semaphore_signal(barrier, inc=1, device_id=(there, partner), device_id_type=MESH)

    loads[0].wait()
    loads[1].wait()

    chunk = rows // max(1, rows // 288)
    if rows % chunk or chunk % 16:
        chunk = rows

    def in_chunks(step):
        if chunk == rows:
            step(pl.ds(0, rows))
        else:

            @pl.loop(0, rows // chunk)
            def _(at):
                step(pl.ds(pl.multiple_of(at * chunk, chunk), chunk))

    def project(ready, which):
        return jnp.dot(ready, weights[which], preferred_element_type=F32)

    loads[2].wait()
    loads[3].wait()

    def left_copy(up, far, source, at):
        part = pl.ds(pl.multiple_of(at * left_rows, 16), left_rows)
        return pltpu.make_async_remote_copy(
            src_ref=left_all.at[source, part],
            dst_ref=left_all.at[source, part],
            send_sem=left_send_sem.at[up, far - 1, source, at],
            recv_sem=left_recv_sem.at[source, at],
            device_id=(north, reached(up, far) * 2 + core),
            device_id_type=MESH,
        )

    for at in range(pieces):
        part = pl.ds(at * left_rows, left_rows)
        ready = scale_channels(pair_in[part, :].astype(F32), gains[pl.ds(0, 1), :]).astype(BF16)
        ready_ref[part, :] = ready
        left = project(ready, 0) * jax.nn.sigmoid(project(ready, 1))
        left_all[chip, part, :] = left.astype(BF16)
        if at == 0:
            expected = sum(exists(*route).astype(jnp.int32) for route in routes)
            pl.semaphore_wait(barrier, expected + 2 * norths - 1)
        for up, far in routes:

            @pl.when(exists(up, far))
            def _():
                left_copy(up, far, chip, at).start()

    loads[4].wait()
    loads[5].wait()

    def right_chunk(part):
        ready = ready_ref[part, :]
        right = project(ready, 2) * jax.nn.sigmoid(project(ready, 3))
        right = right.astype(BF16)
        right_own[part, :] = right
        rows32[part, :] = right.astype(F32)

    in_chunks(right_chunk)
    right_copy = pltpu.make_async_remote_copy(
        src_ref=right_own,
        dst_ref=right_partner,
        send_sem=right_sem.at[0],
        recv_sem=right_sem.at[1],
        device_id=(north, partner),
        device_id_type=MESH,
    )
    right_copy.start()
    for line in range(lines):
        right32[line, pl.ds(0, columns), :] = rows32[pl.ds(line, columns, stride=lines), :]

    loads[6].wait()

    def gate_chunk(part):
        gate_ref[part, :] = jax.nn.sigmoid(project(ready_ref[part, :], 4))

    in_chunks(gate_chunk)

    right_copy.wait()
    rows32[...] = right_partner[...].astype(F32)
    for line in range(lines):
        right32[line, pl.ds(columns, columns), :] = rows32[pl.ds(line, columns, stride=lines), :]

    tiles = 2 * columns // LANES
    group = max(g for g in range(1, deep + 1) if deep % g == 0 and (g * tiles <= 36 or g == 1))

    def sums_copy(half, source, at):
        index = source * 2 + core
        return pltpu.make_async_remote_copy(
            src_ref=sums_send.at[source, half, at],
            dst_ref=sums_all.at[north, index % ratio, at],
            send_sem=sums_send_sem.at[source, half, at],
            recv_sem=sums_recv_sem.at[north, index % ratio, at],
            device_id=(index // ratio, partner if half else east),
            device_id_type=MESH,
        )

    def owned(source):
        return (source * 2 + core) // ratio == north

    def partial_sums(source, at):
        left32[...] = left_all[
            source, pl.ds(pl.multiple_of(at * left_rows, 16), left_rows), :
        ].astype(F32)
        for first in range(0, deep, group):

            def term(line, totals):
                rights = [right32[line, pl.ds(LANES * t, LANES), :] for t in range(tiles)]
                new = []
                for i in range(group):
                    row = left32[pl.ds((first + i) * lines + line, LANES, stride=0), :]
                    for t in range(tiles):
                        new.append(totals[i * tiles + t] + row * rights[t])
                return tuple(new)

            zero = jnp.zeros((LANES, width), F32)
            totals = lax.fori_loop(0, lines, term, (zero,) * (group * tiles), unroll=4)
            for i in range(group):
                for t in range(tiles):
                    row = (first + i) * 2 * columns + LANES * t
                    sums32[pl.ds(row, LANES), :] = totals[i * tiles + t]
        for half in range(2):
            for i in range(deep):
                sums_dense[half, pl.ds(i * columns, columns), :] = sums32[
                    pl.ds((2 * i + half) * columns, columns), :
                ]
        sums_send[source, 1, at] = sums_dense[1].astype(BF16)
        sums_copy(1, source, at).start()
        here = owned(source)

        @pl.when(here)
        def _():
            sums_all[north, (source * 2 + core) % ratio, at] = sums_dense[0].astype(BF16)

        @pl.when(jnp.logical_not(here))
        def _():
            sums_send[source, 0, at] = sums_dense[0].astype(BF16)
            sums_copy(0, source, at).start()

    @pl.loop(0, pieces)
    def _(at):
        partial_sums(chip, at)

    @pl.loop(0, chips // 2 * 2)
    def _(turn):
        hop = turn + 2 - 2 * (turn % 2)

        @pl.loop(0, pieces)
        def _(at):
            for up in range(2):
                source = chip - hop if up else chip + hop

                @pl.when(source >= 0 if up else source < chips)
                def _():
                    left_copy(up, 1, source, at).wait_recv()
                    for far in (2, 1):

                        @pl.when(jnp.logical_and(hop % 2 == 0, exists(up, far)))
                        def _():
                            left_copy(up, far, source, at).start()

                    partial_sums(source, at)

    @pl.loop(0, chips)
    def _(source):
        for at in range(pieces):
            for up, far in routes:
                hop = chip - source if up else source - chip
                passed = jnp.logical_and(hop >= 0, hop % 2 == 0)

                @pl.when(jnp.logical_and(passed, exists(up, far)))
                def _():
                    left_copy(up, far, source, at).wait_send()

            sums_copy(1, source, at).wait_send()

            @pl.when(jnp.logical_not(owned(source)))
            def _():
                sums_copy(0, source, at).wait_send()

    loads[7].wait()
    loads[8].wait()
    for block in range(ratio):
        for at in range(pieces):
            for ahead in range(norths):
                origin = lax.rem(north + ahead, norths)
                arrival = pltpu.make_async_remote_copy(
                    src_ref=sums_send.at[0, 0, at],
                    dst_ref=sums_all.at[origin, block, at],
                    send_sem=sums_send_sem.at[0, 0, at],
                    recv_sem=sums_recv_sem.at[origin, block, at],
                    device_id=(origin, partner),
                    device_id_type=MESH,
                )
                if ahead:
                    arrival.wait_recv()
                else:

                    @pl.when(core != block % 2)
                    def _():
                        arrival.wait_recv()

            total = sums_all[0, block, at].astype(F32)
            for origin in range(1, norths):
                total = total + sums_all[origin, block, at].astype(F32)
            sums32[pl.ds(0, sum_rows), :] = total
            for i in range(deep):
                first = block * columns + at * deep + i
                rows32[pl.ds(first, columns, stride=lines), :] = sums32[
                    pl.ds(i * columns, columns), :
                ]

    def out_chunk(part):
        mixed = (rows32[part, :] * (lines * norths) ** (-0.5)).astype(BF16).astype(F32)
        scaled = scale_channels(mixed, gains[pl.ds(8, 1), :]).astype(BF16)
        out_ref[part, :] = (project(scaled, 5) * gate_ref[part, :]).astype(BF16)

    in_chunks(out_chunk)


def body(pair_rows, in_gain, left_weight, right_weight, left_gate, right_gate, mid_gain, out_weight, out_gate):
    lines, columns, width = pair_rows.shape
    norths, easts = lax.axis_size("north"), lax.axis_size("east")
    rows = lines * columns
    chips, ratio = easts // 2, lines // columns
    pieces = pieces_of(lines, columns)
    left_rows, sum_rows = rows // pieces, columns * columns // pieces
    dma = pltpu.SemaphoreType.DMA
    out = pl.pallas_call(
        functools.partial(kernel, norths, easts, lines, columns),
        out_shape=pltpu.VMEM((rows, width), BF16),
        in_specs=[pl.BlockSpec(memory_space=pl.ANY)] * 9,
        out_specs=pl.BlockSpec(memory_space=pltpu.VMEM),
        scratch_shapes=[
            pltpu.VMEM((rows, width), BF16),
            pltpu.VMEM((16, width), F32),
            pltpu.VMEM((6, width, width), BF16),
            pltpu.VMEM((rows, width), F32),
            pltpu.VMEM((rows, width), BF16),
            pltpu.VMEM((rows, width), F32),
            pltpu.VMEM((chips, rows, width), BF16),
            pltpu.VMEM((left_rows, width), F32),
            pltpu.VMEM((rows, width), BF16),
            pltpu.VMEM((rows, width), BF16),
            pltpu.VMEM((lines, 2 * columns, width), F32),
            pltpu.VMEM((2 * sum_rows, width), F32),
            pltpu.VMEM((2, sum_rows, width), F32),
            pltpu.VMEM((chips, 2, pieces, sum_rows, width), BF16),
            pltpu.VMEM((norths, ratio, pieces, sum_rows, width), BF16),
            dma((9,)),
            dma((2, 2, chips, pieces)),
            dma((chips, pieces)),
            dma((2,)),
            dma((chips, 2, pieces)),
            dma((norths, ratio, pieces)),
        ],
        compiler_params=pltpu.CompilerParams(collective_id=0, has_side_effects=True),
        name="triangle",
    )(
        pair_rows.transpose(1, 0, 2).reshape(rows, width),
        in_gain.reshape(1, -1),
        left_weight,
        right_weight,
        left_gate,
        right_gate,
        mid_gain.reshape(1, -1),
        out_weight,
        out_gate,
    )
    return out.reshape(columns, lines, width).transpose(1, 0, 2)


def solution(mesh):
    placed = (P("north", "east", None), P(), P(), P(), P(), P(), P(), P(), P())
    return jax.shard_map(
        body, mesh=mesh, in_specs=placed, out_specs=P("north", "east", None), check_vma=False
    )
```

```python
import functools

import jax
import jax.numpy as jnp
from jax import lax
from jax.experimental import pallas as pl
from jax.experimental.pallas import tpu as pltpu
from jax.sharding import PartitionSpec as P

MESH = pl.DeviceIdType.MESH
F32 = jnp.float32
BF16 = jnp.bfloat16
LANES = 8


def scale_channels(values, channel_gain):
    centred = values - jnp.mean(values, axis=-1, keepdims=True)
    return (
        centred
        * lax.rsqrt(jnp.mean(centred * centred, axis=-1, keepdims=True) + 1e-05)
        * channel_gain
    )


def pieces_of(lines, columns):
    for pieces in (1,):
        if columns % pieces == 0 and all(
            columns // pieces * side % 16 == 0 for side in (lines, columns)
        ):
            return pieces
    return 1


def kernel(
    norths,
    easts,
    lines,
    columns,
    pair_hbm,
    in_gain_hbm,
    left_weight_hbm,
    right_weight_hbm,
    left_gate_hbm,
    right_gate_hbm,
    mid_gain_hbm,
    out_weight_hbm,
    out_gate_hbm,
    out_ref,
    pair_in,
    gains,
    weights,
    rows32,
    ready_ref,
    gate_ref,
    left_all,
    left32,
    right_own,
    right_partner,
    right32,
    sums32,
    sums_dense,
    sums_send,
    sums_all,
    load_sem,
    left_send_sem,
    left_recv_sem,
    right_sem,
    sums_send_sem,
    sums_recv_sem,
):
    rows, width = pair_in.shape
    chips = easts // 2
    ratio = lines // columns
    pieces = pieces_of(lines, columns)
    deep = columns // pieces
    left_rows, sum_rows = deep * lines, deep * columns

    north = lax.axis_index("north")
    east = lax.axis_index("east")
    chip = east // 2
    core = east % 2
    partner = chip * 2 + 1 - core

    loads = [
        (pair_hbm, pair_in),
        (in_gain_hbm, gains.at[pl.ds(0, 1)]),
        (left_weight_hbm, weights.at[0]),
        (left_gate_hbm, weights.at[1]),
        (right_weight_hbm, weights.at[2]),
        (right_gate_hbm, weights.at[3]),
        (out_gate_hbm, weights.at[4]),
        (out_weight_hbm, weights.at[5]),
        (mid_gain_hbm, gains.at[pl.ds(8, 1)]),
    ]
    loads = [
        pltpu.make_async_copy(source, target, load_sem.at[at])
        for at, (source, target) in enumerate(loads)
    ]
    for load in loads:
        load.start()

    barrier = pltpu.get_barrier_semaphore()
    routes = [(up, far) for far in (2, 1) for up in range(2)]

    def reached(up, far):
        return chip + far if up else chip - far

    def exists(up, far):
        return reached(up, far) < chips if up else reached(up, far) >= 0

    for up, far in routes:

        @pl.when(exists(up, far))
        def _():
            pl.semaphore_signal(
                barrier,
                inc=1,
                device_id=(north, reached(up, far) * 2 + core),
                device_id_type=MESH,
            )

    for step in range(norths):
        there = lax.rem(north + step, norths)
        if step:
            pl.semaphore_signal(barrier, inc=1, device_id=(there, east), device_id_type=MESH)
        pl.semaphore_signal(barrier, inc=1, device_id=(there, partner), device_id_type=MESH)

    loads[0].wait()
    loads[1].wait()

    chunk = rows // max(1, rows // 288)
    if rows % chunk or chunk % 16:
        chunk = rows

    def in_chunks(step):
        if chunk == rows:
            step(pl.ds(0, rows))
        else:

            @pl.loop(0, rows // chunk)
            def _(at):
                step(pl.ds(pl.multiple_of(at * chunk, chunk), chunk))

    def project(ready, which):
        return jnp.dot(ready, weights[which], preferred_element_type=F32)

    loads[2].wait()
    loads[3].wait()

    def left_copy(up, far, source, at):
        part = pl.ds(pl.multiple_of(at * left_rows, 16), left_rows)
        return pltpu.make_async_remote_copy(
            src_ref=left_all.at[source, part],
            dst_ref=left_all.at[source, part],
            send_sem=left_send_sem.at[up, far - 1, source, at],
            recv_sem=left_recv_sem.at[source, at],
            device_id=(north, reached(up, far) * 2 + core),
            device_id_type=MESH,
        )

    for at in range(pieces):
        part = pl.ds(at * left_rows, left_rows)
        ready = scale_channels(pair_in[part, :].astype(F32), gains[pl.ds(0, 1), :]).astype(BF16)
        ready_ref[part, :] = ready
        left = project(ready, 0) * jax.nn.sigmoid(project(ready, 1))
        left_all[chip, part, :] = left.astype(BF16)
        if at == 0:
            expected = sum(exists(*route).astype(jnp.int32) for route in routes)
            pl.semaphore_wait(barrier, expected + 2 * norths - 1)
        for up, far in routes:

            @pl.when(exists(up, far))
            def _():
                left_copy(up, far, chip, at).start()

    loads[4].wait()
    loads[5].wait()

    def right_chunk(part):
        ready = ready_ref[part, :]
        right = project(ready, 2) * jax.nn.sigmoid(project(ready, 3))
        right = right.astype(BF16)
        right_own[part, :] = right
        rows32[part, :] = right.astype(F32)

    in_chunks(right_chunk)
    right_copy = pltpu.make_async_remote_copy(
        src_ref=right_own,
        dst_ref=right_partner,
        send_sem=right_sem.at[0],
        recv_sem=right_sem.at[1],
        device_id=(north, partner),
        device_id_type=MESH,
    )
    right_copy.start()
    for line in range(lines):
        right32[line, pl.ds(0, columns), :] = rows32[pl.ds(line, columns, stride=lines), :]

    loads[6].wait()

    def gate_chunk(part):
        gate_ref[part, :] = jax.nn.sigmoid(project(ready_ref[part, :], 4))

    in_chunks(gate_chunk)

    right_copy.wait()
    rows32[...] = right_partner[...].astype(F32)
    for line in range(lines):
        right32[line, pl.ds(columns, columns), :] = rows32[pl.ds(line, columns, stride=lines), :]

    tiles = 2 * columns // LANES
    group = max(g for g in range(1, deep + 1) if deep % g == 0 and (g * tiles <= 36 or g == 1))

    def sums_copy(half, source, at):
        index = source * 2 + core
        return pltpu.make_async_remote_copy(
            src_ref=sums_send.at[source, half, at],
            dst_ref=sums_all.at[north, index % ratio, at],
            send_sem=sums_send_sem.at[source, half, at],
            recv_sem=sums_recv_sem.at[north, index % ratio, at],
            device_id=(index // ratio, partner if half else east),
            device_id_type=MESH,
        )

    def owned(source):
        return (source * 2 + core) // ratio == north

    def partial_sums(source, at):
        left32[...] = left_all[
            source, pl.ds(pl.multiple_of(at * left_rows, 16), left_rows), :
        ].astype(F32)
        for first in range(0, deep, group):

            def term(line, totals):
                rights = [right32[line, pl.ds(LANES * t, LANES), :] for t in range(tiles)]
                new = []
                for i in range(group):
                    row = left32[pl.ds((first + i) * lines + line, LANES, stride=0), :]
                    for t in range(tiles):
                        new.append(totals[i * tiles + t] + row * rights[t])
                return tuple(new)

            zero = jnp.zeros((LANES, width), F32)
            totals = lax.fori_loop(0, lines, term, (zero,) * (group * tiles), unroll=4)
            for i in range(group):
                for t in range(tiles):
                    row = (first + i) * 2 * columns + LANES * t
                    sums32[pl.ds(row, LANES), :] = totals[i * tiles + t]
        for half in range(2):
            for i in range(deep):
                sums_dense[half, pl.ds(i * columns, columns), :] = sums32[
                    pl.ds((2 * i + half) * columns, columns), :
                ]
        sums_send[source, 1, at] = sums_dense[1].astype(BF16)
        sums_copy(1, source, at).start()
        here = owned(source)

        @pl.when(here)
        def _():
            sums_all[north, (source * 2 + core) % ratio, at] = sums_dense[0].astype(BF16)

        @pl.when(jnp.logical_not(here))
        def _():
            sums_send[source, 0, at] = sums_dense[0].astype(BF16)
            sums_copy(0, source, at).start()

    @pl.loop(0, pieces)
    def _(at):
        partial_sums(chip, at)

    loads[7].wait()
    loads[8].wait()

    def finish():
        for block in range(ratio):
            for at in range(pieces):
                for ahead in range(norths):
                    origin = lax.rem(north + ahead, norths)
                    arrival = pltpu.make_async_remote_copy(
                        src_ref=sums_send.at[0, 0, at],
                        dst_ref=sums_all.at[origin, block, at],
                        send_sem=sums_send_sem.at[0, 0, at],
                        recv_sem=sums_recv_sem.at[origin, block, at],
                        device_id=(origin, partner),
                        device_id_type=MESH,
                    )
                    if ahead:
                        arrival.wait_recv()
                    else:

                        @pl.when(core != block % 2)
                        def _():
                            arrival.wait_recv()

                total = sums_all[0, block, at].astype(F32)
                for origin in range(1, norths):
                    total = total + sums_all[origin, block, at].astype(F32)
                sums32[pl.ds(0, sum_rows), :] = total
                for i in range(deep):
                    first = block * columns + at * deep + i
                    rows32[pl.ds(first, columns, stride=lines), :] = sums32[
                        pl.ds(i * columns, columns), :
                    ]

        def out_chunk(part):
            mixed = (rows32[part, :] * (lines * norths) ** (-0.5)).astype(BF16).astype(F32)
            scaled = scale_channels(mixed, gains[pl.ds(8, 1), :]).astype(BF16)
            out_ref[part, :] = (project(scaled, 5) * gate_ref[part, :]).astype(BF16)

        in_chunks(out_chunk)

    last = chips // 2 * 2
    early = jnp.logical_and((north * ratio) // 2 == chip, ratio <= 2)

    @pl.loop(0, chips // 2 * 2)
    def _(turn):
        hop = turn + 2 - 2 * (turn % 2)

        @pl.when(jnp.logical_and(early, turn == last - 1))
        def _():
            finish()

        @pl.loop(0, pieces)
        def _(at):
            for up in range(2):
                source = chip - hop if up else chip + hop

                @pl.when(source >= 0 if up else source < chips)
                def _():
                    left_copy(up, 1, source, at).wait_recv()
                    for far in (2, 1):

                        @pl.when(jnp.logical_and(hop % 2 == 0, exists(up, far)))
                        def _():
                            left_copy(up, far, source, at).start()

                    partial_sums(source, at)

    @pl.loop(0, chips)
    def _(source):
        for at in range(pieces):
            for up, far in routes:
                hop = chip - source if up else source - chip
                passed = jnp.logical_and(hop >= 0, hop % 2 == 0)

                @pl.when(jnp.logical_and(passed, exists(up, far)))
                def _():
                    left_copy(up, far, source, at).wait_send()

            sums_copy(1, source, at).wait_send()

            @pl.when(jnp.logical_not(owned(source)))
            def _():
                sums_copy(0, source, at).wait_send()

    @pl.when(jnp.logical_not(early))
    def _():
        finish()


def body(pair_rows, in_gain, left_weight, right_weight, left_gate, right_gate, mid_gain, out_weight, out_gate):
    lines, columns, width = pair_rows.shape
    norths, easts = lax.axis_size("north"), lax.axis_size("east")
    rows = lines * columns
    chips, ratio = easts // 2, lines // columns
    pieces = pieces_of(lines, columns)
    left_rows, sum_rows = rows // pieces, columns * columns // pieces
    dma = pltpu.SemaphoreType.DMA
    out = pl.pallas_call(
        functools.partial(kernel, norths, easts, lines, columns),
        out_shape=pltpu.VMEM((rows, width), BF16),
        in_specs=[pl.BlockSpec(memory_space=pl.ANY)] * 9,
        out_specs=pl.BlockSpec(memory_space=pltpu.VMEM),
        scratch_shapes=[
            pltpu.VMEM((rows, width), BF16),
            pltpu.VMEM((16, width), F32),
            pltpu.VMEM((6, width, width), BF16),
            pltpu.VMEM((rows, width), F32),
            pltpu.VMEM((rows, width), BF16),
            pltpu.VMEM((rows, width), F32),
            pltpu.VMEM((chips, rows, width), BF16),
            pltpu.VMEM((left_rows, width), F32),
            pltpu.VMEM((rows, width), BF16),
            pltpu.VMEM((rows, width), BF16),
            pltpu.VMEM((lines, 2 * columns, width), F32),
            pltpu.VMEM((2 * sum_rows, width), F32),
            pltpu.VMEM((2, sum_rows, width), F32),
            pltpu.VMEM((chips, 2, pieces, sum_rows, width), BF16),
            pltpu.VMEM((norths, ratio, pieces, sum_rows, width), BF16),
            dma((9,)),
            dma((2, 2, chips, pieces)),
            dma((chips, pieces)),
            dma((2,)),
            dma((chips, 2, pieces)),
            dma((norths, ratio, pieces)),
        ],
        compiler_params=pltpu.CompilerParams(collective_id=0, has_side_effects=True),
        name="triangle",
    )(
        pair_rows.transpose(1, 0, 2).reshape(rows, width),
        in_gain.reshape(1, -1),
        left_weight,
        right_weight,
        left_gate,
        right_gate,
        mid_gain.reshape(1, -1),
        out_weight,
        out_gate,
    )
    return out.reshape(columns, lines, width).transpose(1, 0, 2)


def solution(mesh):
    placed = (P("north", "east", None), P(), P(), P(), P(), P(), P(), P(), P())
    return jax.shard_map(
        body, mesh=mesh, in_specs=placed, out_specs=P("north", "east", None), check_vma=False
    )
```
